16 devices in a mesh: dp: 2 (over y, z), wg: 8 (over x, core).
Axes of the slice: x: 4, y: 2, z: 1, core: 2. Of those that a mesh axis runs over, the one named last changes fastest.
The devices are a block of a 4x4x8 slice.
Arguments:
- hidden_in: bfloat16 [96, 384, 2048], P(('dp', 'wg')), parts along dimension 0
- ln_g: float32 [2, 2048], replicated
- ln_b: float32 [2, 2048], replicated
- w_qkv: bfloat16 [2, 2048, 3, 32, 64], P(None, 'wg')
- b_qkv: float32 [2, 3, 32, 64], replicated
- w_out: bfloat16 [2, 32, 64, 2048], P(None, None, None, 'wg')
- b_out: float32 [2, 2048], replicated
- w_up: bfloat16 [2, 2048, 8192], P(None, 'wg')
- b_up: float32 [2, 8192], replicated
- w_down: bfloat16 [2, 8192, 2048], P(None, None, 'wg')
- b_down: float32 [2, 2048], replicated
- lnf_g: float32 [2048], replicated
- lnf_b: float32 [2048], replicated
Outputs:
- output: bfloat16 [96, 384, 2048], P(('dp', 'wg')), parts along dimension 0
There are 2 independent parts. The reference program is written for one: setup_inputs(seed, part) draws one part's arguments, and reference() takes and returns one part's arrays. A program takes and returns all parts, laid end to end along the dimension named above; an argument that names none is the same for every part.
All inputs are finite; a program needn't handle non-finite values.
Results may differ from the reference program's by a relative error of at most 0.0107003.
Values are sent between devices in bfloat16 or wider.
A program may use at most 768 MiB of HBM per device.

```python
import jax
import jax.numpy as jnp
from jax import lax

MODEL_DIM = 2048
HEADS = 32
HEAD_DIM = 64
FF_DIM = 8192
LAYERS = 2
SEQ_LEN = 384
BATCH = 48

EPS = 1e-5
ATTN_WIDTH = HEADS * HEAD_DIM


def setup_inputs(seed: int = 0, part: int = 0) -> dict:
    keys = jax.random.split(jax.random.key(seed), 14)
    hidden = jax.random.normal(jax.random.fold_in(keys[0], part), (BATCH, SEQ_LEN, MODEL_DIM), jnp.float32)
    slot_scale = jnp.array([1.5, 1.5, 1.0], jnp.float32).reshape(1, 1, 3, 1, 1)
    w_qkv = jax.random.normal(keys[1], (LAYERS, MODEL_DIM, 3, HEADS, HEAD_DIM), jnp.float32) * slot_scale * MODEL_DIM ** -0.5
    b_qkv = 0.5 * jax.random.normal(keys[2], (LAYERS, 3, HEADS, HEAD_DIM), jnp.float32)
    w_out = jax.random.normal(keys[3], (LAYERS, HEADS, HEAD_DIM, MODEL_DIM), jnp.float32) * ATTN_WIDTH ** -0.5
    b_out = 0.3 * jax.random.normal(keys[4], (LAYERS, MODEL_DIM), jnp.float32)
    w_up = jax.random.normal(keys[5], (LAYERS, MODEL_DIM, FF_DIM), jnp.float32) * MODEL_DIM ** -0.5
    b_up = 0.5 * jax.random.normal(keys[6], (LAYERS, FF_DIM), jnp.float32)
    w_down = jax.random.normal(keys[7], (LAYERS, FF_DIM, MODEL_DIM), jnp.float32) * FF_DIM ** -0.5
    b_down = 0.3 * jax.random.normal(keys[8], (LAYERS, MODEL_DIM), jnp.float32)
    ln_g = 1.0 + 0.3 * jax.random.normal(keys[9], (LAYERS, MODEL_DIM), jnp.float32)
    ln_b = 0.3 * jax.random.normal(keys[10], (LAYERS, MODEL_DIM), jnp.float32)
    lnf_g = 1.0 + 0.3 * jax.random.normal(keys[11], (MODEL_DIM,), jnp.float32)
    lnf_b = 0.3 * jax.random.normal(keys[12], (MODEL_DIM,), jnp.float32)
    return {'hidden_in': hidden.astype(jnp.bfloat16), 'ln_g': ln_g, 'ln_b': ln_b,
            'w_qkv': w_qkv.astype(jnp.bfloat16), 'b_qkv': b_qkv,
            'w_out': w_out.astype(jnp.bfloat16), 'b_out': b_out,
            'w_up': w_up.astype(jnp.bfloat16), 'b_up': b_up,
            'w_down': w_down.astype(jnp.bfloat16), 'b_down': b_down,
            'lnf_g': lnf_g, 'lnf_b': lnf_b}


def layer_norm(rows, gain, shift):
    centered = rows - rows.mean(axis=-1, keepdims=True)
    variance = (centered * centered).mean(axis=-1, keepdims=True)
    return centered * lax.rsqrt(variance + EPS) * gain + shift


def reference(hidden_in, ln_g, ln_b, w_qkv, b_qkv, w_out, b_out, w_up, b_up, w_down, b_down, lnf_g, lnf_b):
    positions = jnp.arange(SEQ_LEN)
    causal = positions[:, None] >= positions[None, :]
    score_scale = HEAD_DIM ** -0.5

    def one_layer(hidden, params):
        norm_gain, norm_shift, qkv_weight, qkv_bias, out_weight, out_bias, up_weight, up_bias, down_weight, down_bias = params
        normed = layer_norm(hidden.astype(jnp.float32), norm_gain, norm_shift).astype(jnp.bfloat16)
        qkv_flat = jnp.dot(normed, qkv_weight.reshape(MODEL_DIM, 3 * ATTN_WIDTH), preferred_element_type=jnp.float32)
        qkv_all = (qkv_flat.reshape(SEQ_LEN, 3, HEADS, HEAD_DIM) + qkv_bias).astype(jnp.bfloat16).astype(jnp.float32)
        scores = jnp.einsum('qhe,khe->hqk', qkv_all[:, 0], qkv_all[:, 1]) * score_scale
        scores = jnp.where(causal, scores, -1e30)
        attn_probs = jax.nn.softmax(scores, axis=-1).astype(jnp.bfloat16).astype(jnp.float32)
        mixed = jnp.einsum('hqk,khe->qhe', attn_probs, qkv_all[:, 2]).astype(jnp.bfloat16)
        attn_proj = jnp.dot(mixed.reshape(SEQ_LEN, ATTN_WIDTH), out_weight.reshape(ATTN_WIDTH, MODEL_DIM), preferred_element_type=jnp.float32)
        up_proj = jnp.dot(normed, up_weight, preferred_element_type=jnp.float32) + up_bias
        gelu_out = jax.nn.gelu(up_proj, approximate=True).astype(jnp.bfloat16)
        down_proj = jnp.dot(gelu_out, down_weight, preferred_element_type=jnp.float32)
        updated = hidden.astype(jnp.float32) + attn_proj + out_bias + down_proj + down_bias
        return updated.astype(jnp.bfloat16), None

    params = (ln_g, ln_b, w_qkv, b_qkv, w_out, b_out, w_up, b_up, w_down, b_down)

    def one_sequence(sequence):
        final, _ = lax.scan(one_layer, sequence, params)
        return layer_norm(final.astype(jnp.float32), lnf_g, lnf_b).astype(jnp.bfloat16)

    return lax.map(one_sequence, hidden_in)
```

```python
import functools

import jax
import jax.numpy as jnp
from jax import lax
from jax.experimental import pallas as pl
from jax.experimental.pallas import tpu as pltpu
from jax.sharding import PartitionSpec as P

EPS = 1e-5
MESH = pl.DeviceIdType.MESH
SLOTS = 7
FLOWS = 9
TO_RIGHT, TO_LEFT, LEFT_AGAIN, PAIR_NEAR, PAIR_FAR, CORE_OWN, CORE_BEFORE, CORE_NEAR, CORE_FAR = range(FLOWS)
FREE_RIGHT, FREE_LEFT, FREE_CORE, FREE_PAIR = range(4)
LOG2_E = 1.4426950408889634


def layer_norm(rows, gain, shift):
    centered = rows - rows.mean(axis=-1, keepdims=True)
    variance = (centered * centered).mean(axis=-1, keepdims=True)
    return centered * lax.rsqrt(variance + EPS) * gain + shift


def dot(lhs, rhs):
    return jnp.dot(lhs, rhs, preferred_element_type=jnp.float32)


def forward_kernel(cfg, hid, wq, wo, wu, wd, bq, bu, bo, gain, shift, last_gain, last_shift, out,
                   acc, act, slots, qkv, mixed, send_sem, recv_sem, load_sem, free_sem, io_sem):
    layers, seqs, seq_len, width, part, head_dim, block, norm_rows = cfg
    parts = width // part
    groups = parts
    chunks = wu.shape[2] // (2 * part)
    per_layer = groups + chunks
    units = layers * per_layer
    half_rows = part // 2

    dp, me = lax.axis_index('dp'), lax.axis_index('wg')
    core = lax.rem(me, 2)
    parity = lax.rem(dp, 2)
    right = (dp, lax.rem(me + 2, parts))
    left = (dp, lax.rem(me + parts - 2, parts))
    partner = (dp, me + 1 - 2 * core)
    pair = (dp + 1 - 2 * parity, me)

    def shard(offset, other=False):
        index = lax.rem(me + parts + offset, parts)
        return index + 1 - 2 * core if other else index

    def piece(unit, index, half=None):
        rows = part if half is None else half_rows
        start = index * part if half is None else index * part + half * half_rows
        return slots.at[lax.rem(unit, SLOTS), pl.ds(pl.multiple_of(start, half_rows), rows), :]

    def remote(flow, unit, ref, target):
        slot = lax.rem(unit, SLOTS)
        return pltpu.make_async_remote_copy(
            src_ref=ref, dst_ref=ref, send_sem=send_sem.at[flow, slot], recv_sem=recv_sem.at[flow, slot],
            device_id=target, device_id_type=MESH)

    def outgoing(flow, unit):
        if flow == TO_RIGHT:
            return remote(flow, unit, piece(unit, me), right)
        if flow == TO_LEFT:
            return remote(flow, unit, piece(unit, me, parity), left)
        if flow == LEFT_AGAIN:
            return remote(flow, unit, piece(unit, shard(2), parity), left)
        if flow == PAIR_NEAR:
            return remote(flow, unit, piece(unit, shard(2), parity), pair)
        if flow == PAIR_FAR:
            return remote(flow, unit, piece(unit, shard(4), parity), pair)
        offset = {CORE_OWN: 0, CORE_BEFORE: -2, CORE_NEAR: 2, CORE_FAR: 4}[flow]
        return remote(flow, unit, piece(unit, shard(offset)), partner)

    def incoming(flow, unit):
        if flow == TO_RIGHT:
            return remote(flow, unit, piece(unit, shard(-2)), right)
        if flow == TO_LEFT:
            return remote(flow, unit, piece(unit, shard(2), parity), left)
        if flow == LEFT_AGAIN:
            return remote(flow, unit, piece(unit, shard(4), parity), left)
        if flow == PAIR_NEAR:
            return remote(flow, unit, piece(unit, shard(2), 1 - parity), pair)
        if flow == PAIR_FAR:
            return remote(flow, unit, piece(unit, shard(4), 1 - parity), pair)
        offset = {CORE_OWN: 0, CORE_BEFORE: -2, CORE_NEAR: 2, CORE_FAR: 4}[flow]
        return remote(flow, unit, piece(unit, shard(offset, other=True)), partner)

    def guarded(stage, unit):
        @pl.when((unit >= 0) & (unit < units))
        def _():
            stage(unit)

    def load_own(unit):
        slot = lax.rem(unit, SLOTS)
        layer, step = unit // per_layer, lax.rem(unit, per_layer)
        rows = pl.ds(pl.multiple_of(me * part, part), part)

        def load(src, first, size):
            pltpu.make_async_copy(src, slots.at[slot, rows, pl.ds(first, size)], load_sem.at[slot]).start()

        @pl.when(step < groups)
        def _():
            load(wq.at[layer, step], 0, 3 * part)
            load(wo.at[layer, pl.ds(pl.multiple_of(step * part, part), part), :], 3 * part, part)

        @pl.when(step >= groups)
        def _():
            first = (step - groups) * 2 * part
            load(wu.at[layer, :, pl.ds(pl.multiple_of(first, 2 * part), 2 * part)], 0, 2 * part)
            for k in range(2):
                load(wd.at[layer, pl.ds(pl.multiple_of(first + k * part, part), part), :], (2 + k) * part, part)

    def send_own(unit):
        ref = piece(unit, me)
        pltpu.make_async_copy(ref, ref, load_sem.at[lax.rem(unit, SLOTS)]).wait()

        @pl.when(unit >= SLOTS)
        def _():
            for which in (FREE_RIGHT, FREE_LEFT, FREE_CORE):
                pl.semaphore_wait(free_sem.at[which], 1)

        for flow in (TO_LEFT, TO_RIGHT, CORE_OWN):
            outgoing(flow, unit).start()

    def pass_near(unit):
        @pl.when(unit >= SLOTS)
        def _():
            pl.semaphore_wait(free_sem.at[FREE_PAIR], 1)

        incoming(TO_LEFT, unit).wait_recv()
        outgoing(LEFT_AGAIN, unit).start()
        outgoing(PAIR_NEAR, unit).start()

    def pass_far(unit):
        incoming(LEFT_AGAIN, unit).wait_recv()
        outgoing(PAIR_FAR, unit).start()
        incoming(TO_RIGHT, unit).wait_recv()
        outgoing(CORE_BEFORE, unit).start()
        incoming(PAIR_NEAR, unit).wait_recv()
        outgoing(CORE_NEAR, unit).start()

    def pass_last(unit):
        incoming(PAIR_FAR, unit).wait_recv()
        outgoing(CORE_FAR, unit).start()

    def arrive(unit):
        for flow in (CORE_OWN, CORE_BEFORE, CORE_NEAR, CORE_FAR):
            incoming(flow, unit).wait_recv()

    def tick(unit):
        guarded(send_own, unit + 5)
        guarded(load_own, unit + 6)
        guarded(pass_last, unit + 1)
        guarded(pass_far, unit + 2)
        guarded(pass_near, unit + 4)
        guarded(arrive, unit)

    def release(unit):
        for flow in range(FLOWS):
            outgoing(flow, unit).wait_send()

        @pl.when(unit + SLOTS < units)
        def _():
            for target, which in ((right, FREE_LEFT), (left, FREE_RIGHT), (partner, FREE_CORE), (pair, FREE_PAIR)):
                pl.semaphore_signal(free_sem.at[which], inc=1, device_id=target, device_id_type=MESH)

    def seq_rows(seq):
        return pl.ds(pl.multiple_of(seq * seq_len, seq_len), seq_len)

    def enter_layer(layer, seq, read):
        def step(i, carry):
            rows = pl.ds(pl.multiple_of(seq * seq_len + i * norm_rows, norm_rows), norm_rows)
            hidden = read(rows).astype(jnp.float32)
            act[rows, :] = layer_norm(hidden, gain[pl.ds(layer, 1), :], shift[pl.ds(layer, 1), :]).astype(jnp.bfloat16)
            acc[rows, :] = hidden + bo[pl.ds(layer, 1), :]
            return carry

        lax.fori_loop(0, seq_len // norm_rows, step, 0)

    causal = (lax.broadcasted_iota(jnp.int32, (block, block), 0)
              >= lax.broadcasted_iota(jnp.int32, (block, block), 1))

    def attention_unit(unit, layer, group):
        w = slots.at[lax.rem(unit, SLOTS)]

        def per_seq(seq, carry):
            rows = seq_rows(seq)
            bias = bq[pl.ds(layer * groups + group, 1), :]
            qkv[...] = (dot(act[rows, :], w[:, :3 * part]) + bias).astype(jnp.bfloat16)
            for head in range(part // head_dim):
                cols = [slice(s * part + head * head_dim, s * part + (head + 1) * head_dim) for s in range(3)]
                for i in range(seq_len // block):
                    mine = slice(i * block, (i + 1) * block)
                    seen = (i + 1) * block
                    scores = lax.dot_general(qkv[mine, cols[0]], qkv[:seen, cols[1]], (((1,), (1,)), ((), ())),
                                             preferred_element_type=jnp.float32)
                    edge = jnp.where(causal, scores[:, i * block:], -1e30)
                    scores = edge if i == 0 else jnp.concatenate([scores[:, :i * block], edge], axis=1)
                    top = scores.max(axis=-1, keepdims=True)
                    weights = jnp.exp2((scores - top) * (head_dim ** -0.5 * LOG2_E))
                    weights = weights * (1.0 / weights.sum(axis=-1, keepdims=True))
                    mixed[mine, head * head_dim:(head + 1) * head_dim] = dot(
                        weights.astype(jnp.bfloat16), qkv[:seen, cols[2]]).astype(jnp.bfloat16)
            for p in range(parts):
                cols = slice(p * part, (p + 1) * part)
                acc[rows, cols] += dot(mixed[...], w[cols, 3 * part:])
            return carry

        lax.fori_loop(0, seqs, per_seq, 0)

    def mlp_unit(unit, layer, chunk):
        w = slots.at[lax.rem(unit, SLOTS)]

        def per_seq(seq, carry):
            rows = seq_rows(seq)
            x = dot(act[rows, :], w[:, :2 * part]) + bu[pl.ds(layer * chunks + chunk, 1), :]
            inner = 0.7978845608028654 * (x + 0.044715 * (x * x * x))
            m = (0.5 * x * (1.0 + jnp.tanh(inner))).astype(jnp.bfloat16)
            for p in range(parts):
                cols = slice(p * part, (p + 1) * part)
                acc[rows, cols] += (dot(m[:, :part], w[cols, 2 * part:3 * part])
                                    + dot(m[:, part:], w[cols, 3 * part:]))
            return carry

        lax.fori_loop(0, seqs, per_seq, 0)

    barrier = pltpu.get_barrier_semaphore()
    for target in (right, left, partner, pair):
        pl.semaphore_signal(barrier, inc=1, device_id=target, device_id_type=MESH)
    read_in = pltpu.make_async_copy(hid, act, io_sem)
    read_in.start()
    load_own(0)
    pl.semaphore_wait(barrier, 4)
    read_in.wait()

    def start_up(i, carry):
        unit = i - 5
        tick(unit)

        @pl.when(i < 5)
        def _():
            enter_layer(0, i, lambda rows: act[rows, :])

        return carry

    lax.fori_loop(0, 5, start_up, 0)
    for seq in range(5, seqs):
        enter_layer(0, seq, lambda rows: act[rows, :])

    def one_layer(layer, carry):
        @pl.when(layer > 0)
        def _():
            def enter(seq, c):
                enter_layer(layer, seq, lambda rows: acc[rows, :].astype(jnp.bfloat16))
                return c

            lax.fori_loop(0, seqs, enter, 0)

        def attention_step(group, c):
            unit = layer * per_layer + group
            tick(unit)
            attention_unit(unit, layer, group)
            release(unit)
            return c

        def mlp_step(chunk, c):
            unit = layer * per_layer + groups + chunk
            tick(unit)
            mlp_unit(unit, layer, chunk)
            release(unit)
            return c

        lax.fori_loop(0, groups, attention_step, 0)
        lax.fori_loop(0, chunks, mlp_step, 0)
        return carry

    lax.fori_loop(0, layers, one_layer, 0)

    def finish(i, carry):
        rows = pl.ds(pl.multiple_of(i * norm_rows, norm_rows), norm_rows)
        hidden = acc[rows, :].astype(jnp.bfloat16).astype(jnp.float32)
        act[rows, :] = layer_norm(hidden, last_gain[...], last_shift[...]).astype(jnp.bfloat16)
        return carry

    lax.fori_loop(0, seqs * seq_len // norm_rows, finish, 0)
    write_out = pltpu.make_async_copy(act, out, io_sem)
    write_out.start()
    write_out.wait()


def solution(mesh):
    row_spec = P(('dp', 'wg'), None, None)
    parts = mesh.shape['wg']

    def local_forward(hidden_in, ln_g, ln_b, w_qkv, b_qkv, w_out, b_out, w_up, b_up, w_down, b_down, lnf_g, lnf_b):
        layers, part, _, heads, head_dim = w_qkv.shape
        seqs, seq_len, width = hidden_in.shape
        ff = w_up.shape[2]
        assert parts == 8 and heads * head_dim == width and part % head_dim == 0
        rows = seqs * seq_len
        block = seq_len // 3
        norm_rows = seq_len // 6
        wq = w_qkv.reshape(layers, part, 3, parts, part).transpose(0, 3, 1, 2, 4).reshape(layers, parts, part, 3 * part)
        bq = b_qkv.reshape(layers, 3, parts, part).transpose(0, 2, 1, 3).reshape(layers * parts, 3 * part)
        bu = b_up.reshape(layers * (ff // (2 * part)), 2 * part)
        vmem = pl.BlockSpec(memory_space=pltpu.VMEM)
        hbm = pl.BlockSpec(memory_space=pl.ANY)
        cfg = (layers, seqs, seq_len, width, part, head_dim, block, norm_rows)
        dma, regular = pltpu.SemaphoreType.DMA, pltpu.SemaphoreType.REGULAR
        out = pl.pallas_call(
            functools.partial(forward_kernel, cfg),
            out_shape=jax.ShapeDtypeStruct((rows, width), jnp.bfloat16),
            in_specs=[hbm] * 5 + [vmem] * 7,
            out_specs=hbm,
            scratch_shapes=[
                pltpu.VMEM((rows, width), jnp.float32),
                pltpu.VMEM((rows, width), jnp.bfloat16),
                pltpu.VMEM((SLOTS, width, 4 * part), jnp.bfloat16),
                pltpu.VMEM((seq_len, 3 * part), jnp.bfloat16),
                pltpu.VMEM((seq_len, part), jnp.bfloat16),
                dma((FLOWS, SLOTS)),
                dma((FLOWS, SLOTS)),
                dma((SLOTS,)),
                regular((4,)),
                dma,
            ],
            compiler_params=pltpu.CompilerParams(
                collective_id=0, has_side_effects=True, vmem_limit_bytes=67_043_328),
            cost_estimate=pl.CostEstimate(
                flops=2 * rows * layers * (4 * width * width + 2 * width * ff),
                bytes_accessed=4 * rows * width, transcendentals=0),
        )(hidden_in.reshape(rows, width), wq, w_out.reshape(layers, width, part), w_up, w_down, bq, bu,
          b_out + b_down, ln_g, ln_b, lnf_g.reshape(1, width), lnf_b.reshape(1, width))
        return out.reshape(seqs, seq_len, width)

    in_specs = (row_spec, P(), P(), P(None, 'wg', None, None, None), P(), P(None, None, None, 'wg'), P(),
                P(None, 'wg', None), P(), P(None, None, 'wg'), P(), P(), P())
    return jax.shard_map(local_forward, mesh=mesh, in_specs=in_specs, out_specs=row_spec, check_vma=False)
```

```python
import functools

import jax
import jax.numpy as jnp
from jax import lax
from jax.experimental import pallas as pl
from jax.experimental.pallas import tpu as pltpu
from jax.sharding import PartitionSpec as P

EPS = 1e-5
MESH = pl.DeviceIdType.MESH
SLOTS = 7
FLOWS = 9
TO_RIGHT, TO_LEFT, LEFT_AGAIN, PAIR_NEAR, PAIR_FAR, CORE_OWN, CORE_BEFORE, CORE_NEAR, CORE_FAR = range(FLOWS)
FREE_RIGHT, FREE_LEFT, FREE_CORE, FREE_PAIR = range(4)
LOG2_E = 1.4426950408889634
GELU_LINEAR = 0.7978845608028654
GELU_CUBIC = GELU_LINEAR * 0.044715
AT_ONCE = 2
MLP_AT_ONCE = 2


def layer_norm(rows, gain, shift):
    centered = rows - rows.mean(axis=-1, keepdims=True)
    variance = (centered * centered).mean(axis=-1, keepdims=True)
    return centered * lax.rsqrt(variance + EPS) * gain + shift


def dot(lhs, rhs):
    return jnp.dot(lhs, rhs, preferred_element_type=jnp.float32)


def forward_kernel(cfg, hid, wq, wo, wu, wd, bq, bu, bo, gain, shift, last_gain, last_shift, out,
                   acc, act, slots, qkv, mixed, send_sem, recv_sem, load_sem, free_sem, io_sem):
    layers, seqs, seq_len, width, part, head_dim, block, norm_rows = cfg
    parts = width // part
    groups = parts
    chunks = wu.shape[2] // (2 * part)
    per_layer = groups + chunks
    units = layers * per_layer
    half_rows = part // 2

    dp, me = lax.axis_index('dp'), lax.axis_index('wg')
    core = lax.rem(me, 2)
    parity = lax.rem(dp, 2)
    right = (dp, lax.rem(me + 2, parts))
    left = (dp, lax.rem(me + parts - 2, parts))
    partner = (dp, me + 1 - 2 * core)
    pair = (dp + 1 - 2 * parity, me)

    def shard(offset, other=False):
        index = lax.rem(me + parts + offset, parts)
        return index + 1 - 2 * core if other else index

    def piece(unit, index, half=None):
        rows = part if half is None else half_rows
        start = index * part if half is None else index * part + half * half_rows
        return slots.at[lax.rem(unit, SLOTS), pl.ds(pl.multiple_of(start, half_rows), rows), :]

    def remote(flow, unit, ref, target):
        slot = lax.rem(unit, SLOTS)
        return pltpu.make_async_remote_copy(
            src_ref=ref, dst_ref=ref, send_sem=send_sem.at[flow, slot], recv_sem=recv_sem.at[flow, slot],
            device_id=target, device_id_type=MESH)

    def outgoing(flow, unit):
        if flow == TO_RIGHT:
            return remote(flow, unit, piece(unit, me), right)
        if flow == TO_LEFT:
            return remote(flow, unit, piece(unit, me, parity), left)
        if flow == LEFT_AGAIN:
            return remote(flow, unit, piece(unit, shard(2), parity), left)
        if flow == PAIR_NEAR:
            return remote(flow, unit, piece(unit, shard(2), parity), pair)
        if flow == PAIR_FAR:
            return remote(flow, unit, piece(unit, shard(4), parity), pair)
        offset = {CORE_OWN: 0, CORE_BEFORE: -2, CORE_NEAR: 2, CORE_FAR: 4}[flow]
        return remote(flow, unit, piece(unit, shard(offset)), partner)

    def incoming(flow, unit):
        if flow == TO_RIGHT:
            return remote(flow, unit, piece(unit, shard(-2)), right)
        if flow == TO_LEFT:
            return remote(flow, unit, piece(unit, shard(2), parity), left)
        if flow == LEFT_AGAIN:
            return remote(flow, unit, piece(unit, shard(4), parity), left)
        if flow == PAIR_NEAR:
            return remote(flow, unit, piece(unit, shard(2), 1 - parity), pair)
        if flow == PAIR_FAR:
            return remote(flow, unit, piece(unit, shard(4), 1 - parity), pair)
        offset = {CORE_OWN: 0, CORE_BEFORE: -2, CORE_NEAR: 2, CORE_FAR: 4}[flow]
        return remote(flow, unit, piece(unit, shard(offset, other=True)), partner)

    def guarded(stage, unit):
        @pl.when((unit >= 0) & (unit < units))
        def _():
            stage(unit)

    def load_own(unit):
        slot = lax.rem(unit, SLOTS)
        layer, step = unit // per_layer, lax.rem(unit, per_layer)
        rows = pl.ds(pl.multiple_of(me * part, part), part)

        def load(src, first, size):
            pltpu.make_async_copy(src, slots.at[slot, rows, pl.ds(first, size)], load_sem.at[slot]).start()

        @pl.when(step < groups)
        def _():
            load(wq.at[layer, step], 0, 3 * part)
            load(wo.at[layer, pl.ds(pl.multiple_of(step * part, part), part), :], 3 * part, part)

        @pl.when(step >= groups)
        def _():
            first = (step - groups) * 2 * part
            load(wu.at[layer, :, pl.ds(pl.multiple_of(first, 2 * part), 2 * part)], 0, 2 * part)
            for k in range(2):
                load(wd.at[layer, pl.ds(pl.multiple_of(first + k * part, part), part), :], (2 + k) * part, part)

    def send_own(unit):
        ref = piece(unit, me)
        pltpu.make_async_copy(ref, ref, load_sem.at[lax.rem(unit, SLOTS)]).wait()

        @pl.when(unit >= SLOTS)
        def _():
            for which in (FREE_RIGHT, FREE_LEFT, FREE_CORE):
                pl.semaphore_wait(free_sem.at[which], 1)

        for flow in (TO_LEFT, TO_RIGHT, CORE_OWN):
            outgoing(flow, unit).start()

    def pass_near(unit):
        @pl.when(unit >= SLOTS)
        def _():
            pl.semaphore_wait(free_sem.at[FREE_PAIR], 1)

        incoming(TO_LEFT, unit).wait_recv()
        outgoing(LEFT_AGAIN, unit).start()
        outgoing(PAIR_NEAR, unit).start()

    def pass_far(unit):
        incoming(LEFT_AGAIN, unit).wait_recv()
        outgoing(PAIR_FAR, unit).start()
        incoming(TO_RIGHT, unit).wait_recv()
        outgoing(CORE_BEFORE, unit).start()
        incoming(PAIR_NEAR, unit).wait_recv()
        outgoing(CORE_NEAR, unit).start()

    def pass_last(unit):
        incoming(PAIR_FAR, unit).wait_recv()
        outgoing(CORE_FAR, unit).start()

    def arrive(unit):
        for flow in (CORE_OWN, CORE_BEFORE, CORE_NEAR, CORE_FAR):
            incoming(flow, unit).wait_recv()

    def tick(unit):
        guarded(send_own, unit + 5)
        guarded(load_own, unit + 6)
        guarded(pass_last, unit + 1)
        guarded(pass_far, unit + 2)
        guarded(pass_near, unit + 4)
        guarded(arrive, unit)

    def release(unit):
        for flow in range(FLOWS):
            outgoing(flow, unit).wait_send()

        @pl.when(unit + SLOTS < units)
        def _():
            for target, which in ((right, FREE_LEFT), (left, FREE_RIGHT), (partner, FREE_CORE), (pair, FREE_PAIR)):
                pl.semaphore_signal(free_sem.at[which], inc=1, device_id=target, device_id_type=MESH)

    def seq_rows(seq):
        return pl.ds(pl.multiple_of(seq * seq_len, seq_len), seq_len)

    def enter_layer(layer, seq, read):
        def step(i, carry):
            rows = pl.ds(pl.multiple_of(seq * seq_len + i * norm_rows, norm_rows), norm_rows)
            hidden = read(rows).astype(jnp.float32)
            act[rows, :] = layer_norm(hidden, gain[pl.ds(layer, 1), :], shift[pl.ds(layer, 1), :]).astype(jnp.bfloat16)
            acc[rows, :] = hidden + bo[pl.ds(layer, 1), :]
            return carry

        lax.fori_loop(0, seq_len // norm_rows, step, 0)

    causal = (lax.broadcasted_iota(jnp.int32, (block, block), 0)
              >= lax.broadcasted_iota(jnp.int32, (block, block), 1))

    def attention_unit(unit, layer, group):
        w = slots.at[lax.rem(unit, SLOTS)]
        heads = range(part // head_dim)
        blocks = range(seq_len // block)

        def project(seq, buf):
            bias = bq[pl.ds(layer * groups + group, 1), :]
            qkv[buf] = (dot(act[seq_rows(seq), :], w[:, :3 * part]) + bias).astype(jnp.bfloat16)

        def scores_of(buf, i):
            mine, seen, scores = slice(i * block, (i + 1) * block), (i + 1) * block, []
            for head in heads:
                q, k = (slice(s * part + head * head_dim, s * part + (head + 1) * head_dim) for s in range(2))
                s = lax.dot_general(qkv[buf, mine, q], qkv[buf, :seen, k], (((1,), (1,)), ((), ())),
                                    preferred_element_type=jnp.float32)
                edge = jnp.where(causal, s[:, i * block:], -1e30)
                scores.append(edge if i == 0 else jnp.concatenate([s[:, :i * block], edge], axis=1))
            return scores

        def mix(buf, i, scores):
            mine, seen = slice(i * block, (i + 1) * block), (i + 1) * block
            tops = [s.max(axis=-1, keepdims=True) for s in scores]
            weights = [jnp.exp2((s - t) * (head_dim ** -0.5 * LOG2_E)) for s, t in zip(scores, tops)]
            scales = [1.0 / e.sum(axis=-1, keepdims=True) for e in weights]
            weights = [(e * c).astype(jnp.bfloat16) for e, c in zip(weights, scales)]
            outs = [dot(e, qkv[buf, :seen, 2 * part + head * head_dim:2 * part + (head + 1) * head_dim])
                    for head, e in zip(heads, weights)]
            mixed[buf, mine, :] = jnp.concatenate([o.astype(jnp.bfloat16) for o in outs], axis=1)

        def attend(buf):
            ready = scores_of(buf, 0)
            for i in blocks:
                later = scores_of(buf, i + 1) if i + 1 < len(blocks) else None
                mix(buf, i, ready)
                ready = later

        def project_out(seq, buf):
            rows = seq_rows(seq)
            for p in range(parts):
                cols = slice(p * part, (p + 1) * part)
                acc[rows, cols] += dot(mixed[buf], w[cols, 3 * part:])

        def some_seqs(i, carry):
            first = i * AT_ONCE
            project(first, 0)
            for k in range(AT_ONCE):
                if k + 1 < AT_ONCE:
                    project(first + k + 1, k + 1)
                attend(k)
                project_out(first + k, k)
            return carry

        lax.fori_loop(0, seqs // AT_ONCE, some_seqs, 0)

    def mlp_unit(unit, layer, chunk):
        w = slots.at[lax.rem(unit, SLOTS)]

        def up(seq):
            return dot(act[seq_rows(seq), :], w[:, :2 * part]) + bu[pl.ds(layer * chunks + chunk, 1), :]

        def gelu(x):
            inner = x * (GELU_LINEAR + GELU_CUBIC * (x * x))
            half = 0.5 * x
            return (half * jnp.tanh(inner) + half).astype(jnp.bfloat16)

        def down(seq, m):
            rows = seq_rows(seq)
            for p in range(parts):
                cols = slice(p * part, (p + 1) * part)
                acc[rows, cols] += (dot(m[:, :part], w[cols, 2 * part:3 * part])
                                    + dot(m[:, part:], w[cols, 3 * part:]))

        def some_seqs(i, carry):
            first = i * MLP_AT_ONCE
            x = up(first)
            for k in range(MLP_AT_ONCE):
                later = up(first + k + 1) if k + 1 < MLP_AT_ONCE else None
                down(first + k, gelu(x))
                x = later
            return carry

        lax.fori_loop(0, seqs // MLP_AT_ONCE, some_seqs, 0)

    barrier = pltpu.get_barrier_semaphore()
    for target in (right, left, partner, pair):
        pl.semaphore_signal(barrier, inc=1, device_id=target, device_id_type=MESH)
    read_in = pltpu.make_async_copy(hid, act, io_sem)
    read_in.start()
    load_own(0)
    pl.semaphore_wait(barrier, 4)
    read_in.wait()

    def start_up(i, carry):
        unit = i - 5
        tick(unit)

        @pl.when(i < 5)
        def _():
            enter_layer(0, i, lambda rows: act[rows, :])

        return carry

    lax.fori_loop(0, 5, start_up, 0)
    for seq in range(5, seqs):
        enter_layer(0, seq, lambda rows: act[rows, :])

    def one_layer(layer, carry):
        @pl.when(layer > 0)
        def _():
            def enter(seq, c):
                enter_layer(layer, seq, lambda rows: acc[rows, :].astype(jnp.bfloat16))
                return c

            lax.fori_loop(0, seqs, enter, 0)

        def attention_step(group, c):
            unit = layer * per_layer + group
            tick(unit)
            attention_unit(unit, layer, group)
            release(unit)
            return c

        def mlp_step(chunk, c):
            unit = layer * per_layer + groups + chunk
            tick(unit)
            mlp_unit(unit, layer, chunk)
            release(unit)
            return c

        lax.fori_loop(0, groups, attention_step, 0)
        lax.fori_loop(0, chunks, mlp_step, 0)
        return carry

    lax.fori_loop(0, layers, one_layer, 0)

    def finish(i, carry):
        rows = pl.ds(pl.multiple_of(i * norm_rows, norm_rows), norm_rows)
        hidden = acc[rows, :].astype(jnp.bfloat16).astype(jnp.float32)
        act[rows, :] = layer_norm(hidden, last_gain[...], last_shift[...]).astype(jnp.bfloat16)
        return carry

    lax.fori_loop(0, seqs * seq_len // norm_rows, finish, 0)
    write_out = pltpu.make_async_copy(act, out, io_sem)
    write_out.start()
    write_out.wait()


def solution(mesh):
    row_spec = P(('dp', 'wg'), None, None)
    parts = mesh.shape['wg']

    def local_forward(hidden_in, ln_g, ln_b, w_qkv, b_qkv, w_out, b_out, w_up, b_up, w_down, b_down, lnf_g, lnf_b):
        layers, part, _, heads, head_dim = w_qkv.shape
        seqs, seq_len, width = hidden_in.shape
        ff = w_up.shape[2]
        assert parts == 8 and heads * head_dim == width and part % head_dim == 0
        rows = seqs * seq_len
        block = seq_len // 3
        norm_rows = seq_len // 6
        wq = w_qkv.reshape(layers, part, 3, parts, part).transpose(0, 3, 1, 2, 4).reshape(layers, parts, part, 3 * part)
        bq = b_qkv.reshape(layers, 3, parts, part).transpose(0, 2, 1, 3).reshape(layers * parts, 3 * part)
        bu = b_up.reshape(layers * (ff // (2 * part)), 2 * part)
        vmem = pl.BlockSpec(memory_space=pltpu.VMEM)
        hbm = pl.BlockSpec(memory_space=pl.ANY)
        cfg = (layers, seqs, seq_len, width, part, head_dim, block, norm_rows)
        dma, regular = pltpu.SemaphoreType.DMA, pltpu.SemaphoreType.REGULAR
        out = pl.pallas_call(
            functools.partial(forward_kernel, cfg),
            out_shape=jax.ShapeDtypeStruct((rows, width), jnp.bfloat16),
            in_specs=[hbm] * 5 + [vmem] * 7,
            out_specs=hbm,
            scratch_shapes=[
                pltpu.VMEM((rows, width), jnp.float32),
                pltpu.VMEM((rows, width), jnp.bfloat16),
                pltpu.VMEM((SLOTS, width, 4 * part), jnp.bfloat16),
                pltpu.VMEM((AT_ONCE, seq_len, 3 * part), jnp.bfloat16),
                pltpu.VMEM((AT_ONCE, seq_len, part), jnp.bfloat16),
                dma((FLOWS, SLOTS)),
                dma((FLOWS, SLOTS)),
                dma((SLOTS,)),
                regular((4,)),
                dma,
            ],
            compiler_params=pltpu.CompilerParams(
                collective_id=0, has_side_effects=True, vmem_limit_bytes=67_043_328),
            cost_estimate=pl.CostEstimate(
                flops=2 * rows * layers * (4 * width * width + 2 * width * ff),
                bytes_accessed=4 * rows * width, transcendentals=0),
        )(hidden_in.reshape(rows, width), wq, w_out.reshape(layers, width, part), w_up, w_down, bq, bu,
          b_out + b_down, ln_g, ln_b, lnf_g.reshape(1, width), lnf_b.reshape(1, width))
        return out.reshape(seqs, seq_len, width)

    in_specs = (row_spec, P(), P(), P(None, 'wg', None, None, None), P(), P(None, None, None, 'wg'), P(),
                P(None, 'wg', None), P(), P(None, None, 'wg'), P(), P(), P())
    return jax.shard_map(local_forward, mesh=mesh, in_specs=in_specs, out_specs=row_spec, check_vma=False)
```

```python
import functools

import jax
import jax.numpy as jnp
from jax import lax
from jax.experimental import pallas as pl
from jax.experimental.pallas import tpu as pltpu
from jax.sharding import PartitionSpec as P

EPS = 1e-5
MESH = pl.DeviceIdType.MESH
SLOTS = 7
FLOWS = 9
TO_RIGHT, TO_LEFT, LEFT_AGAIN, PAIR_NEAR, PAIR_FAR, CORE_OWN, CORE_BEFORE, CORE_NEAR, CORE_FAR = range(FLOWS)
FREE_RIGHT, FREE_LEFT, FREE_CORE, FREE_PAIR = range(4)
LOG2_E = 1.4426950408889634
GELU_LINEAR = 0.7978845608028654
GELU_CUBIC = GELU_LINEAR * 0.044715
AT_ONCE = 3


def layer_norm(rows, gain, shift):
    centered = rows - rows.mean(axis=-1, keepdims=True)
    variance = (centered * centered).mean(axis=-1, keepdims=True)
    return centered * lax.rsqrt(variance + EPS) * gain + shift


def dot(lhs, rhs):
    return jnp.dot(lhs, rhs, preferred_element_type=jnp.float32)


def forward_kernel(cfg, hid, wq, wo, wu, wd, bq, bu, bo, bd, gain, shift, out,
                   acc, act, slots, qkv, mixed, stage, bias_row,
                   send_sem, recv_sem, load_sem, free_sem, stage_sem, io_sem):
    layers, seqs, seq_len, width, part, head_dim, block, norm_rows = cfg
    parts = width // part
    groups = parts
    chunks = wu.shape[2] // (2 * part)
    per_layer = groups + chunks
    units = layers * per_layer
    half_rows = part // 2

    dp, me = lax.axis_index('dp'), lax.axis_index('wg')
    core = lax.rem(me, 2)
    parity = lax.rem(dp, 2)
    right = (dp, lax.rem(me + 2, parts))
    left = (dp, lax.rem(me + parts - 2, parts))
    partner = (dp, me + 1 - 2 * core)
    pair = (dp + 1 - 2 * parity, me)

    def shard(offset, other=False):
        index = lax.rem(me + parts + offset, parts)
        return index + 1 - 2 * core if other else index

    def piece(unit, index, half=None):
        rows = part if half is None else half_rows
        start = index * part if half is None else index * part + half * half_rows
        return slots.at[lax.rem(unit, SLOTS), pl.ds(pl.multiple_of(start, half_rows), rows), :]

    def remote(flow, unit, ref, target):
        slot = lax.rem(unit, SLOTS)
        return pltpu.make_async_remote_copy(
            src_ref=ref, dst_ref=ref, send_sem=send_sem.at[flow, slot], recv_sem=recv_sem.at[flow, slot],
            device_id=target, device_id_type=MESH)

    def outgoing(flow, unit):
        if flow == TO_RIGHT:
            return remote(flow, unit, piece(unit, me), right)
        if flow == TO_LEFT:
            return remote(flow, unit, piece(unit, me, parity), left)
        if flow == LEFT_AGAIN:
            return remote(flow, unit, piece(unit, shard(2), parity), left)
        if flow == PAIR_NEAR:
            return remote(flow, unit, piece(unit, shard(2), parity), pair)
        if flow == PAIR_FAR:
            return remote(flow, unit, piece(unit, shard(4), parity), pair)
        offset = {CORE_OWN: 0, CORE_BEFORE: -2, CORE_NEAR: 2, CORE_FAR: 4}[flow]
        return remote(flow, unit, piece(unit, shard(offset)), partner)

    def incoming(flow, unit):
        if flow == TO_RIGHT:
            return remote(flow, unit, piece(unit, shard(-2)), right)
        if flow == TO_LEFT:
            return remote(flow, unit, piece(unit, shard(2), parity), left)
        if flow == LEFT_AGAIN:
            return remote(flow, unit, piece(unit, shard(4), parity), left)
        if flow == PAIR_NEAR:
            return remote(flow, unit, piece(unit, shard(2), 1 - parity), pair)
        if flow == PAIR_FAR:
            return remote(flow, unit, piece(unit, shard(4), 1 - parity), pair)
        offset = {CORE_OWN: 0, CORE_BEFORE: -2, CORE_NEAR: 2, CORE_FAR: 4}[flow]
        return remote(flow, unit, piece(unit, shard(offset, other=True)), partner)

    def place(unit):
        return unit // per_layer, lax.rem(unit, per_layer)

    def own_rows():
        return pl.ds(pl.multiple_of(me * part, part), part)

    def start_stage(unit):
        layer, step = place(unit)

        @pl.when(step < groups)
        def _():
            for k in range(3):
                rows = pl.ds(pl.multiple_of(k * width + step * part, part), part)
                pltpu.make_async_copy(wq.at[layer, rows, :], stage.at[pl.ds(k * part, part), :], stage_sem).start()

    def load_own(unit):
        slot = lax.rem(unit, SLOTS)
        layer, step = place(unit)

        def load(src, first, size):
            pltpu.make_async_copy(src, slots.at[slot, own_rows(), pl.ds(first, size)], load_sem.at[slot]).start()

        @pl.when(step < groups)
        def _():
            load(wo.at[layer, pl.ds(pl.multiple_of(step * part, part), part), :], 3 * part, part)
            pltpu.make_async_copy(stage, stage, stage_sem).wait()
            for k in range(3):
                slots[slot, own_rows(), k * part:(k + 1) * part] = stage[k * part:(k + 1) * part, :].T

        @pl.when(step >= groups)
        def _():
            first = (step - groups) * 2 * part
            load(wu.at[layer, :, pl.ds(pl.multiple_of(first, 2 * part), 2 * part)], 0, 2 * part)
            for k in range(2):
                load(wd.at[layer, pl.ds(pl.multiple_of(first + k * part, part), part), :], (2 + k) * part, part)

    def send_own(unit):
        slot = lax.rem(unit, SLOTS)
        _, step = place(unit)

        def loaded(cols):
            ref = slots.at[slot, own_rows(), cols]
            pltpu.make_async_copy(ref, ref, load_sem.at[slot]).wait()

        pl.when(step < groups)(lambda: loaded(pl.ds(3 * part, part)))
        pl.when(step >= groups)(lambda: loaded(pl.ds(0, 4 * part)))

        @pl.when(unit >= SLOTS)
        def _():
            for which in (FREE_RIGHT, FREE_LEFT, FREE_CORE):
                pl.semaphore_wait(free_sem.at[which], 1)

        for flow in (TO_LEFT, TO_RIGHT, CORE_OWN):
            outgoing(flow, unit).start()

    def pass_near(unit):
        @pl.when(unit >= SLOTS)
        def _():
            pl.semaphore_wait(free_sem.at[FREE_PAIR], 1)

        incoming(TO_LEFT, unit).wait_recv()
        outgoing(LEFT_AGAIN, unit).start()
        outgoing(PAIR_NEAR, unit).start()

    def pass_far(unit):
        incoming(LEFT_AGAIN, unit).wait_recv()
        outgoing(PAIR_FAR, unit).start()
        incoming(TO_RIGHT, unit).wait_recv()
        outgoing(CORE_BEFORE, unit).start()
        incoming(PAIR_NEAR, unit).wait_recv()
        outgoing(CORE_NEAR, unit).start()

    def pass_last(unit):
        incoming(PAIR_FAR, unit).wait_recv()
        outgoing(CORE_FAR, unit).start()

    def arrive(unit):
        for flow in (CORE_OWN, CORE_BEFORE, CORE_NEAR, CORE_FAR):
            incoming(flow, unit).wait_recv()

    def advance(stage_of, unit, target, most):
        done, wanted = target(unit - 1), target(unit)
        for k in range(1, most + 1):
            later = done + k

            @pl.when((later <= wanted) & (later < units))
            def _():
                stage_of(later)

    def tick_first(unit):
        arrive(unit)
        advance(send_own, unit, lambda t: jnp.minimum(t + 5, 2 * t + 3 + jnp.where(t < 0, 1, 0)), 2)
        advance(pass_far, unit, lambda t: t + 1 + jnp.where(t > 2, 1, 0), 2)

        @pl.when((unit > 0) & (unit + 6 < units))
        def _():
            load_own(unit + 6)

        @pl.when(unit + 7 < units)
        def _():
            start_stage(unit + 7)

    def tick_second(unit):
        advance(pass_near, unit, lambda t: jnp.minimum(t + 4, 2 * t + 2 + jnp.where(t < 0, 1, 0)), 2)

        @pl.when(unit + 1 < units)
        def _():
            pass_last(unit + 1)

    def release(unit):
        for flow in range(FLOWS):
            outgoing(flow, unit).wait_send()

        @pl.when(unit + SLOTS < units)
        def _():
            for target, which in ((right, FREE_LEFT), (left, FREE_RIGHT), (partner, FREE_CORE), (pair, FREE_PAIR)):
                pl.semaphore_signal(free_sem.at[which], inc=1, device_id=target, device_id_type=MESH)

    def seq_rows(seq):
        return pl.ds(pl.multiple_of(seq * seq_len, seq_len), seq_len)

    def enter_layer(layer, seq, read):
        def step(i, carry):
            rows = pl.ds(pl.multiple_of(seq * seq_len + i * norm_rows, norm_rows), norm_rows)
            hidden = read(rows).astype(jnp.float32)
            act[rows, :] = layer_norm(hidden, gain[pl.ds(layer, 1), :], shift[pl.ds(layer, 1), :]).astype(jnp.bfloat16)
            acc[rows, :] = hidden + (bo[pl.ds(layer, 1), :] + bd[pl.ds(layer, 1), :])
            return carry

        lax.fori_loop(0, seq_len // norm_rows, step, 0)

    causal = (lax.broadcasted_iota(jnp.int32, (block, block), 0)
              >= lax.broadcasted_iota(jnp.int32, (block, block), 1))

    def attention_unit(unit, layer, group):
        w = slots.at[lax.rem(unit, SLOTS)]
        heads = range(part // head_dim)
        blocks = range(seq_len // block)

        for k in range(3):
            for head in heads:
                row = (layer * 3 + k) * (width // head_dim) + group * len(heads) + head
                bias_row[:, k * part + head * head_dim:k * part + (head + 1) * head_dim] = bq[pl.ds(row, 1), :]

        def project(seq, buf):
            qkv[buf] = (dot(act[seq_rows(seq), :], w[:, :3 * part]) + bias_row[...]).astype(jnp.bfloat16)

        def scores_of(buf, i):
            mine, seen, scores = slice(i * block, (i + 1) * block), (i + 1) * block, []
            for head in heads:
                q, k = (slice(s * part + head * head_dim, s * part + (head + 1) * head_dim) for s in range(2))
                s = lax.dot_general(qkv[buf, mine, q], qkv[buf, :seen, k], (((1,), (1,)), ((), ())),
                                    preferred_element_type=jnp.float32)
                edge = jnp.where(causal, s[:, i * block:], -1e30)
                scores.append(edge if i == 0 else jnp.concatenate([s[:, :i * block], edge], axis=1))
            return scores

        def mix(buf, i, scores):
            mine, seen = slice(i * block, (i + 1) * block), (i + 1) * block
            tops = [s.max(axis=-1, keepdims=True) for s in scores]
            weights = [jnp.exp2((s - t) * (head_dim ** -0.5 * LOG2_E)) for s, t in zip(scores, tops)]
            scales = [1.0 / e.sum(axis=-1, keepdims=True) for e in weights]
            weights = [(e * c).astype(jnp.bfloat16) for e, c in zip(weights, scales)]
            outs = [dot(e, qkv[buf, :seen, 2 * part + head * head_dim:2 * part + (head + 1) * head_dim])
                    for head, e in zip(heads, weights)]
            mixed[buf, mine, :] = jnp.concatenate([o.astype(jnp.bfloat16) for o in outs], axis=1)

        def attend(buf):
            ready = scores_of(buf, 0)
            for i in blocks:
                later = scores_of(buf, i + 1) if i + 1 < len(blocks) else None
                mix(buf, i, ready)
                ready = later

        def project_out(seq, buf):
            rows = seq_rows(seq)
            for p in range(parts):
                cols = slice(p * part, (p + 1) * part)
                acc[rows, cols] += dot(mixed[buf], w[cols, 3 * part:])

        def some_seqs(i, carry):
            first = i * AT_ONCE
            pl.when(i == 1)(lambda: tick_second(unit))
            project(first, 0)
            for k in range(AT_ONCE):
                if k + 1 < AT_ONCE:
                    project(first + k + 1, k + 1)
                attend(k)
                project_out(first + k, k)
            return carry

        lax.fori_loop(0, seqs // AT_ONCE, some_seqs, 0)

    def mlp_unit(unit, layer, chunk):
        w = slots.at[lax.rem(unit, SLOTS)]

        bias = bu[pl.ds(layer, 1), pl.ds(pl.multiple_of(chunk * 2 * part, 2 * part), 2 * part)]

        def up(seq):
            return dot(act[seq_rows(seq), :], w[:, :2 * part]) + bias

        def gelu(x):
            inner = x * (GELU_LINEAR + GELU_CUBIC * (x * x))
            half = 0.5 * x
            return (half * jnp.tanh(inner) + half).astype(jnp.bfloat16)

        def down(seq, m):
            rows = seq_rows(seq)
            for p in range(parts):
                cols = slice(p * part, (p + 1) * part)
                acc[rows, cols] += (dot(m[:, :part], w[cols, 2 * part:3 * part])
                                    + dot(m[:, part:], w[cols, 3 * part:]))

        def some_seqs(i, carry):
            first = i * AT_ONCE
            pl.when(i == 1)(lambda: tick_second(unit))
            x = up(first)
            for k in range(AT_ONCE):
                later = up(first + k + 1) if k + 1 < AT_ONCE else None
                down(first + k, gelu(x))
                x = later
            return carry

        lax.fori_loop(0, seqs // AT_ONCE, some_seqs, 0)

    barrier = pltpu.get_barrier_semaphore()
    for target in (right, left, partner, pair):
        pl.semaphore_signal(barrier, inc=1, device_id=target, device_id_type=MESH)
    number = [jnp.int32(k) for k in range(SLOTS)]
    read_in = pltpu.make_async_copy(hid, act, io_sem)
    start_stage(number[0])
    read_in.start()
    load_own(number[0])
    start_stage(number[1])
    pl.semaphore_wait(barrier, 4)
    send_own(number[0])
    read_in.wait()

    def enter_first(first, count):
        def enter(seq, c):
            enter_layer(0, seq, lambda rows: act[rows, :])
            return c

        lax.fori_loop(first, first + count, enter, 0)

    def load_next(unit):
        load_own(number[unit])
        if unit + 1 < SLOTS:
            start_stage(number[unit + 1])

    load_next(1)
    enter_first(0, 2)
    pass_near(number[0])
    send_own(number[1])
    load_next(2)
    enter_first(2, 2)
    pass_far(number[0])
    pass_near(number[1])
    send_own(number[2])
    for unit in range(3, SLOTS):
        load_next(unit)
    enter_first(4, seqs - 4)
    pass_last(number[0])

    def one_layer(layer, carry):
        @pl.when(layer > 0)
        def _():
            def enter(seq, c):
                enter_layer(layer, seq, lambda rows: acc[rows, :].astype(jnp.bfloat16))
                return c

            lax.fori_loop(0, seqs, enter, 0)

        def attention_step(group, c):
            unit = layer * per_layer + group
            tick_first(unit)
            attention_unit(unit, layer, group)
            release(unit)
            return c

        def mlp_step(chunk, c):
            unit = layer * per_layer + groups + chunk
            tick_first(unit)
            mlp_unit(unit, layer, chunk)
            release(unit)
            return c

        lax.fori_loop(0, groups, attention_step, 0)
        lax.fori_loop(0, chunks, mlp_step, 0)
        return carry

    lax.fori_loop(0, layers, one_layer, 0)

    def finish(seq, carry):
        rows = seq_rows(seq)
        act[rows, :] = acc[rows, :].astype(jnp.bfloat16)
        pltpu.make_async_copy(act.at[rows, :], out.at[rows, :], io_sem).start()
        return carry

    lax.fori_loop(0, seqs, finish, 0)
    pltpu.make_async_copy(act, out, io_sem).wait()


def last_norm_kernel(hidden, gain, shift, out):
    out[...] = layer_norm(hidden[...].astype(jnp.float32), gain[...], shift[...]).astype(out.dtype)


def solution(mesh):
    row_spec = P(('dp', 'wg'), None, None)
    parts = mesh.shape['wg']

    def local_forward(hidden_in, ln_g, ln_b, w_qkv, b_qkv, w_out, b_out, w_up, b_up, w_down, b_down, lnf_g, lnf_b):
        layers, part, _, heads, head_dim = w_qkv.shape
        seqs, seq_len, width = hidden_in.shape
        ff = w_up.shape[2]
        assert parts == 8 and heads * head_dim == width and part % head_dim == 0
        rows = seqs * seq_len
        block = seq_len // 3
        norm_rows = seq_len // 6
        wq = w_qkv.transpose(0, 2, 3, 4, 1).reshape(layers, 3 * width, part)
        bq = b_qkv.reshape(layers * 3 * heads, head_dim)
        vmem = pl.BlockSpec(memory_space=pltpu.VMEM)
        hbm = pl.BlockSpec(memory_space=pl.ANY)
        cfg = (layers, seqs, seq_len, width, part, head_dim, block, norm_rows)
        dma, regular = pltpu.SemaphoreType.DMA, pltpu.SemaphoreType.REGULAR
        hidden = pl.pallas_call(
            functools.partial(forward_kernel, cfg),
            out_shape=jax.ShapeDtypeStruct((rows, width), jnp.bfloat16),
            in_specs=[hbm] * 5 + [vmem] * 6,
            out_specs=hbm,
            scratch_shapes=[
                pltpu.VMEM((rows, width), jnp.float32),
                pltpu.VMEM((rows, width), jnp.bfloat16),
                pltpu.VMEM((SLOTS, width, 4 * part), jnp.bfloat16),
                pltpu.VMEM((AT_ONCE, seq_len, 3 * part), jnp.bfloat16),
                pltpu.VMEM((AT_ONCE, seq_len, part), jnp.bfloat16),
                pltpu.VMEM((3 * part, part), jnp.bfloat16),
                pltpu.VMEM((1, 3 * part), jnp.float32),
                dma((FLOWS, SLOTS)),
                dma((FLOWS, SLOTS)),
                dma((SLOTS,)),
                regular((4,)),
                dma,
                dma,
            ],
            compiler_params=pltpu.CompilerParams(
                collective_id=0, has_side_effects=True, vmem_limit_bytes=67_043_328),
            cost_estimate=pl.CostEstimate(
                flops=2 * rows * layers * (4 * width * width + 2 * width * ff),
                bytes_accessed=4 * rows * width, transcendentals=0),
        )(hidden_in.reshape(rows, width), wq, w_out.reshape(layers, width, part), w_up, w_down, bq, b_up,
          b_out, b_down, ln_g, ln_b)
        tile = seq_len // 2
        one = pl.BlockSpec((1, width), lambda i: (0, 0))
        tiles = pl.BlockSpec((tile, width), lambda i: (i, 0))
        out = pl.pallas_call(
            last_norm_kernel,
            grid=(rows // tile,),
            out_shape=jax.ShapeDtypeStruct((rows, width), jnp.bfloat16),
            in_specs=[tiles, one, one],
            out_specs=tiles,
        )(hidden, lnf_g.reshape(1, width), lnf_b.reshape(1, width))
        return out.reshape(seqs, seq_len, width)

    in_specs = (row_spec, P(), P(), P(None, 'wg', None, None, None), P(), P(None, None, None, 'wg'), P(),
                P(None, 'wg', None), P(), P(None, None, 'wg'), P(), P(), P())
    return jax.shard_map(local_forward, mesh=mesh, in_specs=in_specs, out_specs=row_spec, check_vma=False)
```
